16 devices in a mesh: dp: 2 (over y, z), tp: 8 (over x, core).
Axes of the slice: x: 4, y: 2, z: 1, core: 2. Of those that a mesh axis runs over, the one named last changes fastest.
The devices are a block of a 4x4x8 slice.
Arguments:
- x: bfloat16 [4096, 4096], P(('dp', 'tp')), parts along dimension 0
- w_gate: bfloat16 [4096, 16384], P(None, 'tp')
- w_up: bfloat16 [4096, 16384], P(None, 'tp')
- w_down: bfloat16 [16384, 4096], P('tp')
Outputs:
- output: bfloat16 [4096, 4096], P(('dp', 'tp')), parts along dimension 0
There are 2 independent parts. The reference program is written for one: setup_inputs(seed, part) draws one part's arguments, and reference() takes and returns one part's arrays. A program takes and returns all parts, laid end to end along the dimension named above; an argument that names none is the same for every part.
All inputs are finite; a program needn't handle non-finite values.
Results may differ from the reference program's by a relative error of at most 0.016.
Values are sent between devices in bfloat16 or wider.
A program may use at most 768 MiB of HBM per device.

```python
import jax
import jax.numpy as jnp

ROWS = 2048
D = 4096
FF = 16384


def setup_inputs(seed: int = 0, part: int = 0) -> dict:
    kx, kg, ku, kd = jax.random.split(jax.random.key(seed), 4)
    drawn = {
        "x": jax.random.normal(jax.random.fold_in(kx, part), (ROWS, D), jnp.float32),
        "w_gate": jax.random.normal(kg, (D, FF), jnp.float32) * D**-0.5,
        "w_up": jax.random.normal(ku, (D, FF), jnp.float32) * D**-0.5,
        "w_down": jax.random.normal(kd, (FF, D), jnp.float32) * FF**-0.5,
    }
    return {k: v.astype(jnp.bfloat16) for k, v in drawn.items()}


def reference(x, w_gate, w_up, w_down):
    gate = jnp.dot(x, w_gate, preferred_element_type=jnp.float32)
    up = jnp.dot(x, w_up, preferred_element_type=jnp.float32)
    hidden = (jax.nn.silu(gate) * up).astype(jnp.bfloat16)
    return jnp.dot(hidden, w_down, preferred_element_type=jnp.float32).astype(jnp.bfloat16)
```

```python
import functools

import jax
import jax.numpy as jnp
from jax import lax
from jax.experimental import pallas as pl
from jax.experimental.pallas import tpu as pltpu
from jax.sharding import PartitionSpec as P

MESH = pl.DeviceIdType.MESH
BF16, F32 = jnp.bfloat16, jnp.float32
LEFT, RIGHT = 0, 1
TN = 256
TD = 512

STAGES = 6
CHUNKS = STAGES + 2


def kernel(
    n_tp, x_ref, wg_ref, wu_ref, wd_ref,
    own_ref, pt_ref, fl_ref, fr_ref, g_ref, xp_ref, u_ref, ps_ref,
    xv, wguv, wdv, h, ownv, tsend, trecv, psv, uv,
    ag_s, ag_r, dx_s, dx_r, dt_s, dt_r, rs_s, rs_r, lx, wg_sem, wu_sem, wd_sem, own_sem, ps_sem, u_sem,
):
    me = lax.axis_index("tp")
    core = lax.rem(me, 2)
    partner = me + 1 - 2 * core
    to = (lax.rem(me + n_tp - 2, n_tp), lax.rem(me + 2, n_tp))
    rows, d = x_ref.shape
    half, q = rows // 2, rows // 4
    nt, nd = wguv.shape[0], wdv.shape[0]

    def remote(src, dst, send, recv, target):
        return pltpu.make_async_remote_copy(
            src_ref=src, dst_ref=dst, send_sem=send, recv_sem=recv, device_id={"tp": target}, device_id_type=MESH
        )

    def ag(way, s):
        if s in (0, 1):
            src = x_ref.at[pl.ds((s + 2 * way) * q, q)]
        elif s in (2, 3):
            src = g_ref.at[s - 2, pl.ds(way * q, q)]
        else:
            src = x_ref.at[pl.ds((s - 4 + 2 * (1 - way)) * q, q)]
        return remote(src, g_ref.at[s, pl.ds(way * q, q)], ag_s.at[way, s], ag_r.at[way, s], to[way])

    def ag_landed(way, s):
        at = g_ref.at[s, pl.ds(way * q, q)]
        remote(at, at, ag_s.at[way, s], ag_r.at[way, s], to[way]).wait_recv()

    def dx_own(i):
        at = pl.ds(i * half, half)
        return remote(x_ref.at[at], xp_ref.at[at], dx_s.at[STAGES + i], dx_r.at[STAGES + i], partner)

    def dx(s):
        return remote(
            g_ref.at[s, pl.ds(0, half)], g_ref.at[s, pl.ds(half, half)], dx_s.at[s], dx_r.at[s], partner
        )

    def dt(j):
        return remote(tsend, trecv.at[lax.rem(j, 2)], dt_s.at[j], dt_r.at[j], partner)

    def dt_own(i):
        j = i * (CHUNKS - 1)
        return remote(tsend, pt_ref.at[pl.ds(i * half, half)], dt_s.at[j], dt_r.at[j], partner)

    def rs(way, s):
        if s in (0, 1):
            part = 1 - way
            dst = fl_ref.at[pl.ds(s * q, q)] if way == RIGHT else fr_ref.at[pl.ds((2 + s) * q, q)]
        elif s in (2, 3):
            part = way
            dst = u_ref.at[s - 2, pl.ds((1 - way) * q, q)]
        else:
            part = 1 - way
            dst = fl_ref.at[pl.ds((s - 2) * q, q)] if way == RIGHT else fr_ref.at[pl.ds((s - 4) * q, q)]
        return remote(ps_ref.at[s, pl.ds(part * q, q)], dst, rs_s.at[way, s], rs_r.at[way, s], to[way])

    def load_x(j, part):
        at = pl.ds(part * half, half)
        return pltpu.make_async_copy(g_ref.at[j - 1, at], xv.at[lax.rem(j, 2), at], lx.at[part])

    def load_own(i, part):
        src = xp_ref if part else x_ref
        return pltpu.make_async_copy(
            src.at[pl.ds(i * half, half)], xv.at[i, pl.ds(part * half, half)], lx.at[part]
        )

    def load_w(w_ref, part, n, sem):
        return pltpu.make_async_copy(
            w_ref.at[:, pl.ds(n * TN, TN)], wguv.at[n, :, pl.ds(part * TN, TN)], sem.at[n]
        )

    def load_wd(n):
        return pltpu.make_async_copy(wd_ref.at[:, pl.ds(n * TD, TD)], wdv.at[n], wd_sem.at[n])

    def keep_own(i):
        return pltpu.make_async_copy(ownv, own_ref.at[pl.ds(i * half, half)], own_sem.at[0])

    def keep_sum(s):
        return pltpu.make_async_copy(psv, ps_ref.at[s], ps_sem.at[0])

    def load_u(s):
        return pltpu.make_async_copy(u_ref.at[s], uv, u_sem.at[0])

    barrier = pltpu.get_barrier_semaphore()
    for other in (*to, partner):
        pl.semaphore_signal(barrier, inc=1, device_id={"tp": other}, device_id_type=MESH)
    load_own(0, 0).start()
    for n in range(2):
        load_w(wg_ref, 0, n, wg_sem).start()
        load_w(wu_ref, 1, n, wu_sem).start()
    pl.semaphore_wait(barrier, 3)
    dx_own(0).start()
    for s in (0, 1):
        for way in (LEFT, RIGHT):
            ag(way, s).start()
    dx_own(1).start()
    for n in range(2, nt):
        load_w(wg_ref, 0, n, wg_sem).start()
        load_w(wu_ref, 1, n, wu_sem).start()
    for n in range(nd):
        load_wd(n).start()
    dx_own(0).wait_recv()
    load_own(0, 1).start()

    def add_terms(j, upstream):
        def body(c, _):
            at = pl.ds(pl.multiple_of(c * TD, TD), TD)
            total = ownv[:, at] + trecv[lax.rem(j, 2), :, at].astype(F32)
            if upstream:
                total = total + uv[:, at].astype(F32)
            psv[:, at] = total.astype(BF16)
            return 0

        lax.fori_loop(0, d // TD, body, 0)

    def chunk(j, _):
        slot = lax.rem(j, 2)
        before = j - 1
        for part in range(2):
            at = pl.ds(part * half, half)
            pltpu.make_async_copy(g_ref.at[0, at], xv.at[slot, at], lx.at[part]).wait()

        def gate_up(n, _):
            @pl.when(j == 0)
            def _():
                load_w(wg_ref, 0, n, wg_sem).wait()
                load_w(wu_ref, 1, n, wu_sem).wait()

            @pl.when(jnp.logical_and(n == 1, j >= 1))
            def _():
                @pl.when(j == 1)
                def _():
                    dt_own(0).start()
                    keep_own(0).start()

                @pl.when(j > 1)
                def _():
                    dt(before).start()

            @pl.when(jnp.logical_and(n == 4, j >= 6))
            def _():
                for s in (2, 3):
                    @pl.when(j == s + 4)
                    def _():
                        for way in (LEFT, RIGHT):
                            rs(way, s).wait_recv()
                        load_u(s - 2).start()

            @pl.when(jnp.logical_and(n == 5, j >= 1))
            def _():
                @pl.when(j == 1)
                def _():
                    dt_own(0).wait()
                    keep_own(0).wait()

                @pl.when(jnp.logical_and(j > 1, j < 6))
                def _():
                    dt(before).wait()
                    add_terms(before, False)

                @pl.when(j >= 6)
                def _():
                    dt(before).wait()
                    load_u(0).wait()
                    add_terms(before, True)

            @pl.when(jnp.logical_and(n == 6, j >= 2))
            def _():
                keep_sum(j - 2).start()

            @pl.when(jnp.logical_and(n == 7, j >= 2))
            def _():
                keep_sum(j - 2).wait()
                for at, stages in ((2, (0,)), (4, (2,)), (5, (3, 1)), (6, (4,)), (7, (5,))):
                    @pl.when(j == at)
                    def _():
                        for s in stages:
                            for way in (LEFT, RIGHT):
                                rs(way, s).start()

            both = jnp.dot(xv[slot], wguv[n], preferred_element_type=F32)
            gate, up = both[:, :TN], both[:, TN:]
            h[:, pl.ds(pl.multiple_of(n * TN, TN), TN)] = (gate * jax.nn.sigmoid(gate) * up).astype(BF16)
            return 0

        lax.fori_loop(0, nt, gate_up, 0)

        def down(n, _):
            @pl.when(j == 0)
            def _():
                load_wd(n).wait()

            @pl.when(jnp.logical_and(n == 1, j < STAGES))
            def _():
                for way in (LEFT, RIGHT):
                    ag_landed(way, j)
                dx(j).start()
                for s in (0, 1):
                    @pl.when(j == s)
                    def _():
                        for way in (LEFT, RIGHT):
                            ag(way, s + 2).start()

                @pl.when(j == 1)
                def _():
                    for s in (4, 5):
                        for way in (LEFT, RIGHT):
                            ag(way, s).start()

            @pl.when(n == nd - 3)
            def _():
                @pl.when(j < STAGES)
                def _():
                    dx(j).wait_recv()
                    for part in range(2):
                        load_x(j + 1, part).start()

                @pl.when(j == STAGES)
                def _():
                    dx_own(1).wait_recv()
                    for part in range(2):
                        load_own(1, part).start()

            at = pl.ds(pl.multiple_of(n * TD, TD), TD)
            term = jnp.dot(h[...], wdv[n], preferred_element_type=F32)
            ownv[:, at] = term[:half]
            tsend[:, at] = term[half:].astype(BF16)
            return 0

        lax.fori_loop(0, nd, down, 0)
        return 0

    lax.fori_loop(0, CHUNKS, chunk, 0)

    for way in (LEFT, RIGHT):
        for s in (0, 1, 4):
            rs(way, s).wait_recv()
    dt_own(1).start()
    keep_own(1).start()
    for s in range(STAGES):
        for way in (LEFT, RIGHT):
            ag(way, s).wait_send()
        dx(s).wait_send()
    for i in range(2):
        dx_own(i).wait_send()
    dt_own(1).wait()
    keep_own(1).wait()
    for s in range(STAGES):
        for way in (LEFT, RIGHT):
            rs(way, s).wait_send()
    for way in (LEFT, RIGHT):
        rs(way, 5).wait_recv()


def solution(mesh):
    n_tp = mesh.shape["tp"]

    def step(x, w_gate, w_up, w_down):
        rows, d = x.shape
        f = w_gate.shape[1]
        half = rows // 2
        nt, nd = f // TN, d // TD
        shape = jax.ShapeDtypeStruct
        outs = [
            shape((rows, d), F32),
            shape((rows, d), BF16),
            shape((rows, d), BF16),
            shape((rows, d), BF16),
            shape((STAGES, rows, d), BF16),
            shape((rows, d), BF16),
            shape((2, half, d), BF16),
            shape((STAGES, half, d), BF16),
        ]
        dma = pltpu.SemaphoreType.DMA
        own, pt, fl, fr, *_ = pl.pallas_call(
            functools.partial(kernel, n_tp),
            out_shape=outs,
            in_specs=[pl.BlockSpec(memory_space=pl.ANY)] * 4,
            out_specs=[pl.BlockSpec(memory_space=pl.ANY)] * len(outs),
            scratch_shapes=[
                pltpu.VMEM((2, rows, d), BF16),
                pltpu.VMEM((nt, d, 2 * TN), BF16),
                pltpu.VMEM((nd, f, TD), BF16),
                pltpu.VMEM((rows, f), BF16),
                pltpu.VMEM((half, d), F32),
                pltpu.VMEM((half, d), BF16),
                pltpu.VMEM((2, half, d), BF16),
                pltpu.VMEM((half, d), BF16),
                pltpu.VMEM((half, d), BF16),
                dma((2, STAGES)), dma((2, STAGES)),
                dma((CHUNKS,)), dma((CHUNKS,)),
                dma((CHUNKS,)), dma((CHUNKS,)),
                dma((2, STAGES)), dma((2, STAGES)),
                dma((2,)), dma((nt,)), dma((nt,)), dma((nd,)), dma((1,)), dma((1,)), dma((1,)),
            ],
            compiler_params=pltpu.CompilerParams(
                collective_id=0, has_side_effects=True, vmem_limit_bytes=67043328
            ),
            name="mlp_block",
        )(x, w_gate, w_up, w_down)
        total = own + pt.astype(F32) + fl.astype(F32) + fr.astype(F32)
        return total.astype(BF16)

    return jax.shard_map(
        step,
        mesh=mesh,
        in_specs=(P(("dp", "tp"), None), P(None, "tp"), P(None, "tp"), P("tp", None)),
        out_specs=P(("dp", "tp"), None),
        check_vma=False,
    )
```

```python
import functools

import jax
import jax.numpy as jnp
from jax import lax
from jax.experimental import pallas as pl
from jax.experimental.pallas import tpu as pltpu
from jax.sharding import PartitionSpec as P

MESH = pl.DeviceIdType.MESH
BF16, F32 = jnp.bfloat16, jnp.float32
LEFT, RIGHT = 0, 1
TN = 256
TD = 512
UNROLL = 2

STAGES = 6
CHUNKS = STAGES + 2


def kernel(
    n_tp, x_ref, wg_ref, wu_ref, wd_ref,
    own_ref, pt_ref, fl_ref, fr_ref, g_ref, xp_ref, u_ref, ps_ref,
    xv, wguv, wdv, h, ownv, tsend, trecv, psv, uv,
    ag_s, ag_r, dx_s, dx_r, dt_s, dt_r, rs_s, rs_r, lx, wg_sem, wu_sem, wd_sem, own_sem, ps_sem, u_sem,
):
    me = lax.axis_index("tp")
    core = lax.rem(me, 2)
    partner = me + 1 - 2 * core
    to = (lax.rem(me + n_tp - 2, n_tp), lax.rem(me + 2, n_tp))
    rows, d = x_ref.shape
    half, q = rows // 2, rows // 4
    nt, nd = wguv.shape[0], wdv.shape[0]

    def remote(src, dst, send, recv, target):
        return pltpu.make_async_remote_copy(
            src_ref=src, dst_ref=dst, send_sem=send, recv_sem=recv, device_id={"tp": target}, device_id_type=MESH
        )

    def ag(way, s):
        if s in (0, 1):
            src = x_ref.at[pl.ds((s + 2 * way) * q, q)]
        elif s in (2, 3):
            src = g_ref.at[s - 2, pl.ds(way * q, q)]
        else:
            src = x_ref.at[pl.ds((s - 4 + 2 * (1 - way)) * q, q)]
        return remote(src, g_ref.at[s, pl.ds(way * q, q)], ag_s.at[way, s], ag_r.at[way, s], to[way])

    def ag_landed(way, s):
        at = g_ref.at[s, pl.ds(way * q, q)]
        remote(at, at, ag_s.at[way, s], ag_r.at[way, s], to[way]).wait_recv()

    def dx_own(i):
        at = pl.ds(i * half, half)
        return remote(x_ref.at[at], xp_ref.at[at], dx_s.at[STAGES + i], dx_r.at[STAGES + i], partner)

    def dx(s):
        return remote(
            g_ref.at[s, pl.ds(0, half)], g_ref.at[s, pl.ds(half, half)], dx_s.at[s], dx_r.at[s], partner
        )

    def dt(j):
        return remote(tsend, trecv.at[lax.rem(j, 2)], dt_s.at[j], dt_r.at[j], partner)

    def dt_own(i):
        j = i * (CHUNKS - 1)
        return remote(tsend, pt_ref.at[pl.ds(i * half, half)], dt_s.at[j], dt_r.at[j], partner)

    def rs(way, s):
        if s in (0, 1):
            part = 1 - way
            dst = fl_ref.at[pl.ds(s * q, q)] if way == RIGHT else fr_ref.at[pl.ds((2 + s) * q, q)]
        elif s in (2, 3):
            part = way
            dst = u_ref.at[s - 2, pl.ds((1 - way) * q, q)]
        else:
            part = 1 - way
            dst = fl_ref.at[pl.ds((s - 2) * q, q)] if way == RIGHT else fr_ref.at[pl.ds((s - 4) * q, q)]
        return remote(ps_ref.at[s, pl.ds(part * q, q)], dst, rs_s.at[way, s], rs_r.at[way, s], to[way])

    def load_x(j, part):
        at = pl.ds(part * half, half)
        return pltpu.make_async_copy(g_ref.at[j - 1, at], xv.at[lax.rem(j, 2), at], lx.at[part])

    def load_own(i, part):
        src = xp_ref if part else x_ref
        return pltpu.make_async_copy(
            src.at[pl.ds(i * half, half)], xv.at[i, pl.ds(part * half, half)], lx.at[part]
        )

    def load_w(w_ref, part, n, sem):
        return pltpu.make_async_copy(
            w_ref.at[:, pl.ds(n * TN, TN)], wguv.at[n, :, pl.ds(part * TN, TN)], sem.at[n]
        )

    def load_wd(n):
        return pltpu.make_async_copy(wd_ref.at[:, pl.ds(n * TD, TD)], wdv.at[n], wd_sem.at[n])

    def load_gate_up(m):
        for i in range(UNROLL):
            load_w(wg_ref, 0, m * UNROLL + i, wg_sem).start()
            load_w(wu_ref, 1, m * UNROLL + i, wu_sem).start()

    def load_down(m):
        for i in range(UNROLL):
            load_wd(m * UNROLL + i).start()

    def keep_own(i):
        return pltpu.make_async_copy(ownv, own_ref.at[pl.ds(i * half, half)], own_sem.at[0])

    def keep_sum(s):
        return pltpu.make_async_copy(psv, ps_ref.at[s], ps_sem.at[0])

    def load_u(s):
        return pltpu.make_async_copy(u_ref.at[s], uv, u_sem.at[0])

    barrier = pltpu.get_barrier_semaphore()
    for other in (*to, partner):
        pl.semaphore_signal(barrier, inc=1, device_id={"tp": other}, device_id_type=MESH)
    load_own(0, 0).start()
    load_gate_up(0)
    pl.semaphore_wait(barrier, 3)
    dx_own(0).start()
    for s in (0, 1):
        for way in (LEFT, RIGHT):
            ag(way, s).start()
    dx_own(1).start()
    dx_own(0).wait_recv()
    load_own(0, 1).start()
    load_gate_up(1)

    def add_terms(j, upstream):
        def body(c, _):
            at = pl.ds(pl.multiple_of(c * TD, TD), TD)
            total = ownv[:, at] + trecv[lax.rem(j, 2), :, at].astype(F32)
            if upstream:
                total = total + uv[:, at].astype(F32)
            psv[:, at] = total.astype(BF16)
            return 0

        lax.fori_loop(0, d // TD, body, 0)

    def chunk(j, _):
        slot = lax.rem(j, 2)
        before = j - 1
        for part in range(2):
            at = pl.ds(part * half, half)
            pltpu.make_async_copy(g_ref.at[0, at], xv.at[slot, at], lx.at[part]).wait()

        def gate_up(m, _):
            @pl.when(j == 0)
            def _():
                for i in range(UNROLL):
                    load_w(wg_ref, 0, m * UNROLL + i, wg_sem).wait()
                    load_w(wu_ref, 1, m * UNROLL + i, wu_sem).wait()

                @pl.when(m + 2 < nt // UNROLL)
                def _():
                    load_gate_up(m + 2)

                @pl.when(m + 2 >= nt // UNROLL)
                def _():
                    load_down(m + 2 - nt // UNROLL)

            @pl.when(jnp.logical_and(m == 1, j >= 1))
            def _():
                @pl.when(j == 1)
                def _():
                    dt_own(0).start()
                    keep_own(0).start()

                @pl.when(j > 1)
                def _():
                    dt(before).start()

            @pl.when(jnp.logical_and(m == 2, j >= 6))
            def _():
                for s in (2, 3):
                    @pl.when(j == s + 4)
                    def _():
                        for way in (LEFT, RIGHT):
                            rs(way, s).wait_recv()
                        load_u(s - 2).start()

            @pl.when(jnp.logical_and(m == 3, j >= 1))
            def _():
                @pl.when(j == 1)
                def _():
                    dt_own(0).wait()
                    keep_own(0).wait()

                @pl.when(jnp.logical_and(j > 1, j < 6))
                def _():
                    dt(before).wait()
                    add_terms(before, False)

                @pl.when(j >= 6)
                def _():
                    dt(before).wait()
                    load_u(0).wait()
                    add_terms(before, True)

            for i in range(UNROLL):
                n = m * UNROLL + i
                both = jnp.dot(xv[slot], wguv[n], preferred_element_type=F32)
                gate, up = both[:, :TN], both[:, TN:]
                h[:, pl.ds(pl.multiple_of(n * TN, TN), TN)] = (gate * jax.nn.sigmoid(gate) * up).astype(BF16)
            return 0

        lax.fori_loop(0, nt // UNROLL, gate_up, 0)

        def down(m, _):
            @pl.when(j == 0)
            def _():
                for i in range(UNROLL):
                    load_wd(m * UNROLL + i).wait()

                @pl.when(m + 2 < nd // UNROLL)
                def _():
                    load_down(m + 2)

            @pl.when(m == 0)
            def _():
                @pl.when(j < STAGES)
                def _():
                    for way in (LEFT, RIGHT):
                        ag_landed(way, j)
                    dx(j).start()
                    for s in (0, 1):
                        @pl.when(j == s)
                        def _():
                            for way in (LEFT, RIGHT):
                                ag(way, s + 2).start()

                    @pl.when(j == 1)
                    def _():
                        for s in (4, 5):
                            for way in (LEFT, RIGHT):
                                ag(way, s).start()

                    load_x(j + 1, 0).start()

                @pl.when(j == STAGES)
                def _():
                    load_own(1, 0).start()

                @pl.when(j >= 2)
                def _():
                    keep_sum(j - 2).start()

            @pl.when(jnp.logical_and(m == 1, j >= 2))
            def _():
                keep_sum(j - 2).wait()
                for at, stages in ((2, (0,)), (4, (2,)), (5, (3, 1)), (6, (4,)), (7, (5,))):
                    @pl.when(j == at)
                    def _():
                        for s in stages:
                            for way in (LEFT, RIGHT):
                                rs(way, s).start()

            @pl.when(m == 2)
            def _():
                @pl.when(j < STAGES)
                def _():
                    dx(j).wait_recv()
                    load_x(j + 1, 1).start()

                @pl.when(j == STAGES)
                def _():
                    dx_own(1).wait_recv()
                    load_own(1, 1).start()

            for i in range(UNROLL):
                n = m * UNROLL + i
                at = pl.ds(pl.multiple_of(n * TD, TD), TD)
                term = jnp.dot(h[...], wdv[n], preferred_element_type=F32)
                ownv[:, at] = term[:half]
                tsend[:, at] = term[half:].astype(BF16)
            return 0

        lax.fori_loop(0, nd // UNROLL, down, 0)
        return 0

    lax.fori_loop(0, CHUNKS, chunk, 0)

    for way in (LEFT, RIGHT):
        for s in (0, 1, 4):
            rs(way, s).wait_recv()
    dt_own(1).start()
    keep_own(1).start()
    for s in range(STAGES):
        for way in (LEFT, RIGHT):
            ag(way, s).wait_send()
        dx(s).wait_send()
    for i in range(2):
        dx_own(i).wait_send()
    dt_own(1).wait()
    keep_own(1).wait()
    for s in range(STAGES):
        for way in (LEFT, RIGHT):
            rs(way, s).wait_send()
    for way in (LEFT, RIGHT):
        rs(way, 5).wait_recv()


def solution(mesh):
    n_tp = mesh.shape["tp"]

    def step(x, w_gate, w_up, w_down):
        rows, d = x.shape
        f = w_gate.shape[1]
        half = rows // 2
        nt, nd = f // TN, d // TD
        shape = jax.ShapeDtypeStruct
        outs = [
            shape((rows, d), F32),
            shape((rows, d), BF16),
            shape((rows, d), BF16),
            shape((rows, d), BF16),
            shape((STAGES, rows, d), BF16),
            shape((rows, d), BF16),
            shape((2, half, d), BF16),
            shape((STAGES, half, d), BF16),
        ]
        dma = pltpu.SemaphoreType.DMA
        own, pt, fl, fr, *_ = pl.pallas_call(
            functools.partial(kernel, n_tp),
            out_shape=outs,
            in_specs=[pl.BlockSpec(memory_space=pl.ANY)] * 4,
            out_specs=[pl.BlockSpec(memory_space=pl.ANY)] * len(outs),
            scratch_shapes=[
                pltpu.VMEM((2, rows, d), BF16),
                pltpu.VMEM((nt, d, 2 * TN), BF16),
                pltpu.VMEM((nd, f, TD), BF16),
                pltpu.VMEM((rows, f), BF16),
                pltpu.VMEM((half, d), F32),
                pltpu.VMEM((half, d), BF16),
                pltpu.VMEM((2, half, d), BF16),
                pltpu.VMEM((half, d), BF16),
                pltpu.VMEM((half, d), BF16),
                dma((2, STAGES)), dma((2, STAGES)),
                dma((CHUNKS,)), dma((CHUNKS,)),
                dma((CHUNKS,)), dma((CHUNKS,)),
                dma((2, STAGES)), dma((2, STAGES)),
                dma((2,)), dma((nt,)), dma((nt,)), dma((nd,)), dma((1,)), dma((1,)), dma((1,)),
            ],
            compiler_params=pltpu.CompilerParams(
                collective_id=0, has_side_effects=True, vmem_limit_bytes=67043328
            ),
            name="mlp_block",
        )(x, w_gate, w_up, w_down)
        total = own + pt.astype(F32) + fl.astype(F32) + fr.astype(F32)
        return total.astype(BF16)

    return jax.shard_map(
        step,
        mesh=mesh,
        in_specs=(P(("dp", "tp"), None), P(None, "tp"), P(None, "tp"), P("tp", None)),
        out_specs=P(("dp", "tp"), None),
        check_vma=False,
    )
```

```python
import functools

import jax
import jax.numpy as jnp
from jax import lax
from jax.experimental import pallas as pl
from jax.experimental.pallas import tpu as pltpu
from jax.sharding import PartitionSpec as P

MESH = pl.DeviceIdType.MESH
BF16, F32 = jnp.bfloat16, jnp.float32
LEFT, RIGHT = 0, 1
TN = 256
TD = 512
UNROLL = 2

STAGES = 6
CHUNKS = STAGES + 2


def kernel(
    n_tp, x_ref, wg_ref, wu_ref, wd_ref,
    y_ref, fl_ref, fr_ref, g_ref, xp_ref, u_ref, ps_ref,
    xv, wguv, wdv, h, ownv, tsend, trecv, uv, last,
    ag_s, ag_r, dx_s, dx_r, dt_s, dt_r, rs_s, rs_r, lx, wg_sem, wu_sem, wd_sem, y_sem, ps_sem, u_sem,
):
    me = lax.axis_index("tp")
    core = lax.rem(me, 2)
    partner = me + 1 - 2 * core
    to = (lax.rem(me + n_tp - 2, n_tp), lax.rem(me + 2, n_tp))
    rows, d = x_ref.shape
    half, q = rows // 2, rows // 4
    nt, nd = wguv.shape[0], wdv.shape[0]

    def remote(src, dst, send, recv, target):
        return pltpu.make_async_remote_copy(
            src_ref=src, dst_ref=dst, send_sem=send, recv_sem=recv, device_id={"tp": target}, device_id_type=MESH
        )

    def ag(way, s):
        if s in (0, 1):
            src = x_ref.at[pl.ds((s + 2 * way) * q, q)]
        elif s in (2, 3):
            src = g_ref.at[s - 2, pl.ds(way * q, q)]
        else:
            src = x_ref.at[pl.ds((s - 4 + 2 * (1 - way)) * q, q)]
        return remote(src, g_ref.at[s, pl.ds(way * q, q)], ag_s.at[way, s], ag_r.at[way, s], to[way])

    def ag_landed(way, s):
        at = g_ref.at[s, pl.ds(way * q, q)]
        remote(at, at, ag_s.at[way, s], ag_r.at[way, s], to[way]).wait_recv()

    def dx_own(i):
        at = pl.ds(i * half, half)
        return remote(x_ref.at[at], xp_ref.at[at], dx_s.at[STAGES + i], dx_r.at[STAGES + i], partner)

    def dx(s):
        return remote(
            g_ref.at[s, pl.ds(0, half)], g_ref.at[s, pl.ds(half, half)], dx_s.at[s], dx_r.at[s], partner
        )

    def dt(j):
        return remote(tsend, trecv.at[lax.rem(j, 2)], dt_s.at[j], dt_r.at[j], partner)

    def rs(way, s):
        if s in (0, 1):
            part = 1 - way
            dst = fl_ref.at[pl.ds(s * q, q)] if way == RIGHT else fr_ref.at[pl.ds((2 + s) * q, q)]
        elif s in (2, 3):
            part = way
            dst = u_ref.at[s - 2, pl.ds((1 - way) * q, q)]
        elif s == 4:
            part = 1 - way
            dst = fl_ref.at[pl.ds(2 * q, q)] if way == RIGHT else fr_ref.at[pl.ds(0, q)]
        else:
            part = 1 - way
            dst = last.at[way]
        return remote(ps_ref.at[s, pl.ds(part * q, q)], dst, rs_s.at[way, s], rs_r.at[way, s], to[way])

    def load_x(j, part):
        at = pl.ds(part * half, half)
        return pltpu.make_async_copy(g_ref.at[j - 1, at], xv.at[lax.rem(j, 2), at], lx.at[part])

    def load_own(i, part):
        src = xp_ref if part else x_ref
        return pltpu.make_async_copy(
            src.at[pl.ds(i * half, half)], xv.at[i, pl.ds(part * half, half)], lx.at[part]
        )

    def load_w(w_ref, part, n, sem):
        return pltpu.make_async_copy(
            w_ref.at[:, pl.ds(n * TN, TN)], wguv.at[n, :, pl.ds(part * TN, TN)], sem.at[n]
        )

    def load_wd(n):
        return pltpu.make_async_copy(wd_ref.at[:, pl.ds(n * TD, TD)], wdv.at[n], wd_sem.at[n])

    def load_gate_up(m):
        for i in range(UNROLL):
            load_w(wg_ref, 0, m * UNROLL + i, wg_sem).start()
            load_w(wu_ref, 1, m * UNROLL + i, wu_sem).start()

    def load_down(m):
        for i in range(UNROLL):
            load_wd(m * UNROLL + i).start()

    def keep_sum(s):
        return pltpu.make_async_copy(trecv.at[lax.rem(s + 1, 2)], ps_ref.at[s], ps_sem.at[0])

    def load_u(s):
        return pltpu.make_async_copy(u_ref.at[s], uv, u_sem.at[0])

    barrier = pltpu.get_barrier_semaphore()
    for other in (*to, partner):
        pl.semaphore_signal(barrier, inc=1, device_id={"tp": other}, device_id_type=MESH)
    load_own(0, 0).start()
    load_gate_up(0)
    pl.semaphore_wait(barrier, 3)
    dx_own(0).start()
    for s in (0, 1):
        for way in (LEFT, RIGHT):
            ag(way, s).start()
    dx_own(1).start()
    dx_own(0).wait_recv()
    load_own(0, 1).start()
    load_gate_up(1)

    def columns(body):
        def step(c, _):
            body(pl.ds(pl.multiple_of(c * TD, TD), TD))
            return 0

        lax.fori_loop(0, d // TD, step, 0)

    def add_terms(j, upstream):
        def body(at):
            total = ownv[1, :, at] + trecv[lax.rem(j, 2), :, at].astype(F32)
            if upstream:
                total = total + uv[:, at].astype(F32)
            trecv[lax.rem(j, 2), :, at] = total.astype(BF16)

        columns(body)

    def add_own(i, part):
        def body(at):
            ownv[i, :, at] = ownv[i, :, at] + part(at).astype(F32)

        columns(body)

    def chunk(j, _):
        slot = lax.rem(j, 2)
        before = j - 1
        for part in range(2):
            at = pl.ds(part * half, half)
            pltpu.make_async_copy(g_ref.at[0, at], xv.at[slot, at], lx.at[part]).wait()

        def gate_up(m, _):
            @pl.when(j == 0)
            def _():
                for i in range(UNROLL):
                    load_w(wg_ref, 0, m * UNROLL + i, wg_sem).wait()
                    load_w(wu_ref, 1, m * UNROLL + i, wu_sem).wait()

                @pl.when(m + 2 < nt // UNROLL)
                def _():
                    load_gate_up(m + 2)

                @pl.when(m + 2 >= nt // UNROLL)
                def _():
                    load_down(m + 2 - nt // UNROLL)

            @pl.when(jnp.logical_and(m == 1, j >= 1))
            def _():
                dt(before).start()

            @pl.when(jnp.logical_and(m == 2, j >= 6))
            def _():
                for s in (2, 3):
                    @pl.when(j == s + 4)
                    def _():
                        for way in (LEFT, RIGHT):
                            rs(way, s).wait_recv()
                        load_u(s - 2).start()

            @pl.when(jnp.logical_and(m == 3, j >= 1))
            def _():
                dt(before).wait()

                @pl.when(j == 1)
                def _():
                    add_own(0, lambda at: trecv[0, :, at])

                @pl.when(jnp.logical_and(j > 1, j < 6))
                def _():
                    add_terms(before, False)

                @pl.when(j >= 6)
                def _():
                    load_u(0).wait()
                    add_terms(before, True)

            for i in range(UNROLL):
                n = m * UNROLL + i
                both = jnp.dot(xv[slot], wguv[n], preferred_element_type=F32)
                gate, up = both[:, :TN], both[:, TN:]
                h[:, pl.ds(pl.multiple_of(n * TN, TN), TN)] = (gate * jax.nn.sigmoid(gate) * up).astype(BF16)
            return 0

        lax.fori_loop(0, nt // UNROLL, gate_up, 0)

        def down(m, _):
            @pl.when(j == 0)
            def _():
                for i in range(UNROLL):
                    load_wd(m * UNROLL + i).wait()

                @pl.when(m + 2 < nd // UNROLL)
                def _():
                    load_down(m + 2)

            @pl.when(m == 0)
            def _():
                @pl.when(j < STAGES)
                def _():
                    for way in (LEFT, RIGHT):
                        ag_landed(way, j)
                    dx(j).start()
                    for s in (0, 1):
                        @pl.when(j == s)
                        def _():
                            for way in (LEFT, RIGHT):
                                ag(way, s + 2).start()

                    @pl.when(j == 1)
                    def _():
                        for s in (4, 5):
                            for way in (LEFT, RIGHT):
                                ag(way, s).start()

                    load_x(j + 1, 0).start()

                @pl.when(j == STAGES)
                def _():
                    load_own(1, 0).start()

                @pl.when(j >= 2)
                def _():
                    keep_sum(j - 2).start()

            @pl.when(jnp.logical_and(m == 1, j >= 2))
            def _():
                keep_sum(j - 2).wait()
                for at, stages in ((2, (0,)), (4, (2,)), (5, (3, 1)), (6, (4,)), (7, (5,))):
                    @pl.when(j == at)
                    def _():
                        for s in stages:
                            for way in (LEFT, RIGHT):
                                rs(way, s).start()

            @pl.when(m == 2)
            def _():
                @pl.when(j < STAGES)
                def _():
                    dx(j).wait_recv()
                    load_x(j + 1, 1).start()

                @pl.when(j == STAGES)
                def _():
                    dx_own(1).wait_recv()
                    load_own(1, 1).start()

            for i in range(UNROLL):
                n = m * UNROLL + i
                at = pl.ds(pl.multiple_of(n * TD, TD), TD)
                term = jnp.dot(h[...], wdv[n], preferred_element_type=F32)
                ownv[lax.min(j, 1), :, at] = term[:half]
                tsend[:, at] = term[half:].astype(BF16)
            return 0

        lax.fori_loop(0, nd // UNROLL, down, 0)
        return 0

    lax.fori_loop(0, CHUNKS, chunk, 0)

    def fetch(src, dst, i):
        return pltpu.make_async_copy(src, dst, lx.at[i])

    def put(i, src):
        return pltpu.make_async_copy(src, y_ref.at[pl.ds(i * q, q)], y_sem.at[i])

    def finish(dst, acc, part, rows_at):
        def body(at):
            dst[:, at] = (ownv[acc, rows_at, at] + part(at).astype(F32)).astype(BF16)

        columns(body)

    top, bottom = pl.ds(0, q), pl.ds(q, q)
    first, second = pl.ds(0, half), pl.ds(half, half)

    for s in (0, 1):
        for way in (LEFT, RIGHT):
            rs(way, s).wait_recv()
    loads = fetch(fl_ref.at[first], xv.at[0, first], 0), fetch(fr_ref.at[second], xv.at[0, second], 1)
    for load in loads:
        load.start()
    for load in loads:
        load.wait()
    dt(CHUNKS - 1).start()
    add_own(0, lambda at: xv[0, first, at])
    add_own(1, lambda at: xv[0, second, at])
    dt(CHUNKS - 1).wait()
    add_own(1, lambda at: trecv[(CHUNKS - 1) % 2, :, at])

    for way in (LEFT, RIGHT):
        rs(way, 4).wait_recv()
    loads = fetch(fr_ref.at[top], xv.at[1, top], 0), fetch(fl_ref.at[pl.ds(half, q)], xv.at[1, bottom], 1)
    for load in loads:
        load.start()
    for load in loads:
        load.wait()
    finish(tsend.at[top], 0, lambda at: xv[1, top, at], top)
    put(0, tsend.at[top]).start()
    finish(tsend.at[bottom], 1, lambda at: xv[1, bottom, at], top)
    put(2, tsend.at[bottom]).start()

    for s in range(STAGES):
        for way in (LEFT, RIGHT):
            ag(way, s).wait_send()
        dx(s).wait_send()
    for i in range(2):
        dx_own(i).wait_send()
    for s in range(STAGES - 1):
        for way in (LEFT, RIGHT):
            rs(way, s).wait_send()
    put(0, tsend.at[top]).wait()
    put(2, tsend.at[bottom]).wait()

    done = trecv.at[0]
    rs(LEFT, 5).wait_recv()
    finish(done.at[top], 0, lambda at: last[LEFT, :, at], bottom)
    put(1, done.at[top]).start()
    rs(RIGHT, 5).wait_recv()
    finish(done.at[bottom], 1, lambda at: last[RIGHT, :, at], bottom)
    put(3, done.at[bottom]).start()
    for way in (LEFT, RIGHT):
        rs(way, 5).wait_send()
    put(1, done.at[top]).wait()
    put(3, done.at[bottom]).wait()


def solution(mesh):
    n_tp = mesh.shape["tp"]

    def step(x, w_gate, w_up, w_down):
        rows, d = x.shape
        f = w_gate.shape[1]
        half = rows // 2
        nt, nd = f // TN, d // TD
        shape = jax.ShapeDtypeStruct
        outs = [
            shape((rows, d), BF16),
            shape((rows, d), BF16),
            shape((rows, d), BF16),
            shape((STAGES, rows, d), BF16),
            shape((rows, d), BF16),
            shape((2, half, d), BF16),
            shape((STAGES, half, d), BF16),
        ]
        dma = pltpu.SemaphoreType.DMA
        y, *_ = pl.pallas_call(
            functools.partial(kernel, n_tp),
            out_shape=outs,
            in_specs=[pl.BlockSpec(memory_space=pl.ANY)] * 4,
            out_specs=[pl.BlockSpec(memory_space=pl.ANY)] * len(outs),
            scratch_shapes=[
                pltpu.VMEM((2, rows, d), BF16),
                pltpu.VMEM((nt, d, 2 * TN), BF16),
                pltpu.VMEM((nd, f, TD), BF16),
                pltpu.VMEM((rows, f), BF16),
                pltpu.VMEM((2, half, d), F32),
                pltpu.VMEM((half, d), BF16),
                pltpu.VMEM((2, half, d), BF16),
                pltpu.VMEM((half, d), BF16),
                pltpu.VMEM((2, rows // 4, d), BF16),
                dma((2, STAGES)), dma((2, STAGES)),
                dma((CHUNKS,)), dma((CHUNKS,)),
                dma((CHUNKS,)), dma((CHUNKS,)),
                dma((2, STAGES)), dma((2, STAGES)),
                dma((2,)), dma((nt,)), dma((nt,)), dma((nd,)), dma((4,)), dma((1,)), dma((1,)),
            ],
            compiler_params=pltpu.CompilerParams(
                collective_id=0, has_side_effects=True, vmem_limit_bytes=67043328
            ),
            name="mlp_block",
        )(x, w_gate, w_up, w_down)
        return y

    return jax.shard_map(
        step,
        mesh=mesh,
        in_specs=(P(("dp", "tp"), None), P(None, "tp"), P(None, "tp"), P("tp", None)),
        out_specs=P(("dp", "tp"), None),
        check_vma=False,
    )
```

```python
import functools

import jax
import jax.numpy as jnp
from jax import lax
from jax.experimental import pallas as pl
from jax.experimental.pallas import tpu as pltpu
from jax.sharding import PartitionSpec as P

MESH = pl.DeviceIdType.MESH
BF16, F32 = jnp.bfloat16, jnp.float32
LEFT, RIGHT = 0, 1
TN = 256
TD = 512
UNROLL = 2

STAGES = 6
CHUNKS = STAGES + 2


def kernel(
    n_tp, x_ref, wg_ref, wu_ref, wd_ref,
    y_ref, fl_ref, fr_ref, g_ref, xp_ref, u_ref, ps_ref,
    xv, wguv, wdv, h, ownv, tsend, uv, last,
    ag_s, ag_r, dx_s, dx_r, dt_s, dt_r, rs_s, rs_r, lx, wg_sem, wu_sem, wd_sem, ps_sem, u_sem,
):
    me = lax.axis_index("tp")
    core = lax.rem(me, 2)
    partner = me + 1 - 2 * core
    to = (lax.rem(me + n_tp - 2, n_tp), lax.rem(me + 2, n_tp))
    rows, d = x_ref.shape
    half, q = rows // 2, rows // 4
    nt, nd = wguv.shape[0], wdv.shape[0]
    trecv = y_ref

    def remote(src, dst, send, recv, target):
        return pltpu.make_async_remote_copy(
            src_ref=src, dst_ref=dst, send_sem=send, recv_sem=recv, device_id={"tp": target}, device_id_type=MESH
        )

    def ag(way, s):
        if s in (0, 1):
            src = x_ref.at[pl.ds((s + 2 * way) * q, q)]
        elif s in (2, 3):
            src = g_ref.at[s - 2, pl.ds(way * q, q)]
        else:
            src = x_ref.at[pl.ds((s - 4 + 2 * (1 - way)) * q, q)]
        return remote(src, g_ref.at[s, pl.ds(way * q, q)], ag_s.at[way, s], ag_r.at[way, s], to[way])

    def ag_landed(way, s):
        at = g_ref.at[s, pl.ds(way * q, q)]
        remote(at, at, ag_s.at[way, s], ag_r.at[way, s], to[way]).wait_recv()

    def dx_own(i):
        at = pl.ds(i * half, half)
        return remote(x_ref.at[at], xp_ref.at[at], dx_s.at[STAGES + i], dx_r.at[STAGES + i], partner)

    def dx(s):
        return remote(
            g_ref.at[s, pl.ds(0, half)], g_ref.at[s, pl.ds(half, half)], dx_s.at[s], dx_r.at[s], partner
        )

    def dt(j):
        return remote(tsend, trecv.at[lax.rem(j, 2)], dt_s.at[j], dt_r.at[j], partner)

    def rs(way, s):
        if s in (0, 1):
            part = 1 - way
            dst = fl_ref.at[pl.ds(s * q, q)] if way == RIGHT else fr_ref.at[pl.ds((2 + s) * q, q)]
        elif s in (2, 3):
            part = way
            dst = u_ref.at[s - 2, pl.ds((1 - way) * q, q)]
        elif s == 4:
            part = 1 - way
            dst = fl_ref.at[pl.ds(2 * q, q)] if way == RIGHT else fr_ref.at[pl.ds(0, q)]
        else:
            part = 1 - way
            dst = last.at[way]
        return remote(ps_ref.at[s, pl.ds(part * q, q)], dst, rs_s.at[way, s], rs_r.at[way, s], to[way])

    def load_x(j, part):
        at = pl.ds(part * half, half)
        return pltpu.make_async_copy(g_ref.at[j - 1, at], xv.at[lax.rem(j, 2), at], lx.at[part])

    def load_own(i, part):
        src = xp_ref if part else x_ref
        return pltpu.make_async_copy(
            src.at[pl.ds(i * half, half)], xv.at[i, pl.ds(part * half, half)], lx.at[part]
        )

    def load_w(w_ref, part, n, sem):
        return pltpu.make_async_copy(
            w_ref.at[:, pl.ds(n * TN, TN)], wguv.at[n, :, pl.ds(part * TN, TN)], sem.at[n]
        )

    def load_wd(n):
        return pltpu.make_async_copy(wd_ref.at[:, pl.ds(n * TD, TD)], wdv.at[n], wd_sem.at[n])

    def load_gate_up(m):
        for i in range(UNROLL):
            load_w(wg_ref, 0, m * UNROLL + i, wg_sem).start()
            load_w(wu_ref, 1, m * UNROLL + i, wu_sem).start()

    def load_down(m):
        for i in range(UNROLL):
            load_wd(m * UNROLL + i).start()

    def keep_sum(s):
        return pltpu.make_async_copy(trecv.at[lax.rem(s + 1, 2)], ps_ref.at[s], ps_sem.at[0])

    def load_u(s):
        return pltpu.make_async_copy(u_ref.at[s], uv, u_sem.at[0])

    barrier = pltpu.get_barrier_semaphore()
    for other in (*to, partner):
        pl.semaphore_signal(barrier, inc=1, device_id={"tp": other}, device_id_type=MESH)
    load_own(0, 0).start()
    load_gate_up(0)
    pl.semaphore_wait(barrier, 3)
    dx_own(0).start()
    for s in (0, 1):
        for way in (LEFT, RIGHT):
            ag(way, s).start()
    dx_own(1).start()
    dx_own(0).wait_recv()
    load_own(0, 1).start()
    load_gate_up(1)

    def columns(body):
        def step(c, _):
            body(pl.ds(pl.multiple_of(c * TD, TD), TD))
            return 0

        lax.fori_loop(0, d // TD, step, 0)

    def add_terms(j, upstream):
        def body(at):
            total = ownv[1, :, at] + trecv[lax.rem(j, 2), :, at].astype(F32)
            if upstream:
                total = total + uv[:, at].astype(F32)
            trecv[lax.rem(j, 2), :, at] = total.astype(BF16)

        columns(body)

    def add_own(i, part):
        def body(at):
            ownv[i, :, at] = ownv[i, :, at] + part(at).astype(F32)

        columns(body)

    def chunk(j, _):
        slot = lax.rem(j, 2)
        before = j - 1
        for part in range(2):
            at = pl.ds(part * half, half)
            pltpu.make_async_copy(g_ref.at[0, at], xv.at[slot, at], lx.at[part]).wait()

        def gate_up(m, _):
            @pl.when(j == 0)
            def _():
                for i in range(UNROLL):
                    load_w(wg_ref, 0, m * UNROLL + i, wg_sem).wait()
                    load_w(wu_ref, 1, m * UNROLL + i, wu_sem).wait()

                @pl.when(m + 2 < nt // UNROLL)
                def _():
                    load_gate_up(m + 2)

                @pl.when(m + 2 >= nt // UNROLL)
                def _():
                    load_down(m + 2 - nt // UNROLL)

            @pl.when(jnp.logical_and(m == 1, j >= 1))
            def _():
                dt(before).start()

            @pl.when(jnp.logical_and(m == 2, j >= 6))
            def _():
                for s in (2, 3):
                    @pl.when(j == s + 4)
                    def _():
                        for way in (LEFT, RIGHT):
                            rs(way, s).wait_recv()
                        load_u(s - 2).start()

            @pl.when(jnp.logical_and(m == 3, j >= 1))
            def _():
                dt(before).wait()

                @pl.when(j == 1)
                def _():
                    add_own(0, lambda at: trecv[0, :, at])

                @pl.when(jnp.logical_and(j > 1, j < 6))
                def _():
                    add_terms(before, False)

                @pl.when(j >= 6)
                def _():
                    load_u(0).wait()
                    add_terms(before, True)

            for i in range(UNROLL):
                n = m * UNROLL + i
                both = jnp.dot(xv[slot], wguv[n], preferred_element_type=F32)
                gate, up = both[:, :TN], both[:, TN:]
                h[:, pl.ds(pl.multiple_of(n * TN, TN), TN)] = (gate * jax.nn.sigmoid(gate) * up).astype(BF16)
            return 0

        lax.fori_loop(0, nt // UNROLL, gate_up, 0)

        def down(m, _):
            @pl.when(j == 0)
            def _():
                for i in range(UNROLL):
                    load_wd(m * UNROLL + i).wait()

                @pl.when(m + 2 < nd // UNROLL)
                def _():
                    load_down(m + 2)

            @pl.when(m == 0)
            def _():
                @pl.when(j < STAGES)
                def _():
                    for way in (LEFT, RIGHT):
                        ag_landed(way, j)
                    dx(j).start()
                    for s in (0, 1):
                        @pl.when(j == s)
                        def _():
                            for way in (LEFT, RIGHT):
                                ag(way, s + 2).start()

                    @pl.when(j == 1)
                    def _():
                        for s in (4, 5):
                            for way in (LEFT, RIGHT):
                                ag(way, s).start()

                    load_x(j + 1, 0).start()

                @pl.when(j == STAGES)
                def _():
                    load_own(1, 0).start()

                @pl.when(j >= 2)
                def _():
                    keep_sum(j - 2).start()

            @pl.when(jnp.logical_and(m == 1, j >= 2))
            def _():
                keep_sum(j - 2).wait()
                for at, stages in ((2, (0,)), (4, (2,)), (5, (3, 1)), (6, (4,)), (7, (5,))):
                    @pl.when(j == at)
                    def _():
                        for s in stages:
                            for way in (LEFT, RIGHT):
                                rs(way, s).start()

            @pl.when(m == 2)
            def _():
                @pl.when(j < STAGES)
                def _():
                    dx(j).wait_recv()
                    load_x(j + 1, 1).start()

                @pl.when(j == STAGES)
                def _():
                    dx_own(1).wait_recv()
                    load_own(1, 1).start()

            for i in range(UNROLL):
                n = m * UNROLL + i
                at = pl.ds(pl.multiple_of(n * TD, TD), TD)
                term = jnp.dot(h[...], wdv[n], preferred_element_type=F32)
                ownv[lax.min(j, 1), :, at] = term[:half]
                tsend[:, at] = term[half:].astype(BF16)
            return 0

        lax.fori_loop(0, nd // UNROLL, down, 0)
        return 0

    lax.fori_loop(0, CHUNKS, chunk, 0)

    def fetch(src, dst, i):
        return pltpu.make_async_copy(src, dst, lx.at[i])

    def finish(dst, acc, part, rows_at):
        def body(at):
            dst[:, at] = (ownv[acc, rows_at, at] + part(at).astype(F32)).astype(BF16)

        columns(body)

    top, bottom = pl.ds(0, q), pl.ds(q, q)
    first, second = pl.ds(0, half), pl.ds(half, half)

    for s in (0, 1):
        for way in (LEFT, RIGHT):
            rs(way, s).wait_recv()
    loads = fetch(fl_ref.at[first], xv.at[0, first], 0), fetch(fr_ref.at[second], xv.at[0, second], 1)
    for load in loads:
        load.start()
    for load in loads:
        load.wait()
    dt(CHUNKS - 1).start()
    add_own(0, lambda at: xv[0, first, at])
    add_own(1, lambda at: xv[0, second, at])
    dt(CHUNKS - 1).wait()
    add_own(1, lambda at: trecv[(CHUNKS - 1) % 2, :, at])

    for way in (LEFT, RIGHT):
        rs(way, 4).wait_recv()
    loads = fetch(fr_ref.at[top], xv.at[1, top], 0), fetch(fl_ref.at[pl.ds(half, q)], xv.at[1, bottom], 1)
    for load in loads:
        load.start()
    for load in loads:
        load.wait()
    finish(y_ref.at[0, top], 0, lambda at: xv[1, top, at], top)
    finish(y_ref.at[1, top], 1, lambda at: xv[1, bottom, at], top)

    for s in range(STAGES):
        for way in (LEFT, RIGHT):
            ag(way, s).wait_send()
        dx(s).wait_send()
    for i in range(2):
        dx_own(i).wait_send()
    for s in range(STAGES - 1):
        for way in (LEFT, RIGHT):
            rs(way, s).wait_send()
    for way in (LEFT, RIGHT):
        rs(way, 5).wait_recv()
        finish(y_ref.at[way, bottom], way, lambda at, way=way: last[way, :, at], bottom)
    for way in (LEFT, RIGHT):
        rs(way, 5).wait_send()


def solution(mesh):
    n_tp = mesh.shape["tp"]

    def step(x, w_gate, w_up, w_down):
        rows, d = x.shape
        f = w_gate.shape[1]
        half = rows // 2
        nt, nd = f // TN, d // TD
        shape = jax.ShapeDtypeStruct
        outs = [
            pltpu.VMEM((2, half, d), BF16),
            shape((rows, d), BF16),
            shape((rows, d), BF16),
            shape((STAGES, rows, d), BF16),
            shape((rows, d), BF16),
            shape((2, half, d), BF16),
            shape((STAGES, half, d), BF16),
        ]
        dma = pltpu.SemaphoreType.DMA
        y, *_ = pl.pallas_call(
            functools.partial(kernel, n_tp),
            out_shape=outs,
            in_specs=[pl.BlockSpec(memory_space=pl.ANY)] * 4,
            out_specs=[pl.BlockSpec(memory_space=pltpu.VMEM)] + [pl.BlockSpec(memory_space=pl.ANY)] * (len(outs) - 1),
            scratch_shapes=[
                pltpu.VMEM((2, rows, d), BF16),
                pltpu.VMEM((nt, d, 2 * TN), BF16),
                pltpu.VMEM((nd, f, TD), BF16),
                pltpu.VMEM((rows, f), BF16),
                pltpu.VMEM((2, half, d), F32),
                pltpu.VMEM((half, d), BF16),
                pltpu.VMEM((half, d), BF16),
                pltpu.VMEM((2, rows // 4, d), BF16),
                dma((2, STAGES)), dma((2, STAGES)),
                dma((CHUNKS,)), dma((CHUNKS,)),
                dma((CHUNKS,)), dma((CHUNKS,)),
                dma((2, STAGES)), dma((2, STAGES)),
                dma((2,)), dma((nt,)), dma((nt,)), dma((nd,)), dma((1,)), dma((1,)),
            ],
            compiler_params=pltpu.CompilerParams(
                collective_id=0, has_side_effects=True, vmem_limit_bytes=64900000
            ),
            name="mlp_block",
        )(x, w_gate, w_up, w_down)
        return y.reshape(rows, d)

    return jax.shard_map(
        step,
        mesh=mesh,
        in_specs=(P(("dp", "tp"), None), P(None, "tp"), P(None, "tp"), P("tp", None)),
        out_specs=P(("dp", "tp"), None),
        check_vma=False,
    )
```

```python
import functools

import jax
import jax.numpy as jnp
from jax import lax
from jax.experimental import pallas as pl
from jax.experimental.pallas import tpu as pltpu
from jax.sharding import PartitionSpec as P

MESH = pl.DeviceIdType.MESH
BF16, F32 = jnp.bfloat16, jnp.float32
LEFT, RIGHT = 0, 1
TN = 256
TD = 512
UNROLL = 2

STAGES = 6
CHUNKS = STAGES + 2


def kernel(
    n_tp, x_ref, wg_ref, wu_ref, wd_ref,
    y_ref, fl_ref, fr_ref, g_ref, xp_ref, u_ref, ps_ref,
    xv, wguv, wdv, h, ownv, tsend, uv, last,
    ag_s, ag_r, dx_s, dx_r, dt_s, dt_r, rs_s, rs_r, lx, wg_sem, wu_sem, wd_sem, ps_sem, u_sem,
):
    me = lax.axis_index("tp")
    core = lax.rem(me, 2)
    partner = me + 1 - 2 * core
    to = (lax.rem(me + n_tp - 2, n_tp), lax.rem(me + 2, n_tp))
    rows, d = x_ref.shape
    half, q = rows // 2, rows // 4
    nt, nd = wguv.shape[0], wdv.shape[0]
    trecv = y_ref

    def remote(src, dst, send, recv, target):
        return pltpu.make_async_remote_copy(
            src_ref=src, dst_ref=dst, send_sem=send, recv_sem=recv, device_id={"tp": target}, device_id_type=MESH
        )

    def ag(way, s):
        if s in (0, 1):
            src = x_ref.at[pl.ds((s + 2 * way) * q, q)]
        elif s in (2, 3):
            src = g_ref.at[s - 2, pl.ds(way * q, q)]
        else:
            src = x_ref.at[pl.ds((s - 4 + 2 * (1 - way)) * q, q)]
        return remote(src, g_ref.at[s, pl.ds(way * q, q)], ag_s.at[way, s], ag_r.at[way, s], to[way])

    def ag_landed(way, s):
        at = g_ref.at[s, pl.ds(way * q, q)]
        remote(at, at, ag_s.at[way, s], ag_r.at[way, s], to[way]).wait_recv()

    def dx_own(i):
        at = pl.ds(i * half, half)
        return remote(x_ref.at[at], xp_ref.at[at], dx_s.at[STAGES + i], dx_r.at[STAGES + i], partner)

    def dx(s):
        return remote(
            g_ref.at[s, pl.ds(0, half)], g_ref.at[s, pl.ds(half, half)], dx_s.at[s], dx_r.at[s], partner
        )

    def dt(j):
        return remote(tsend, trecv.at[lax.rem(j, 2)], dt_s.at[j], dt_r.at[j], partner)

    def rs(way, s):
        if s in (0, 1):
            part = 1 - way
            dst = fl_ref.at[pl.ds(s * q, q)] if way == RIGHT else fr_ref.at[pl.ds((2 + s) * q, q)]
        elif s in (2, 3):
            part = way
            dst = u_ref.at[s - 2, pl.ds((1 - way) * q, q)]
        elif s == 4:
            part = 1 - way
            dst = fl_ref.at[pl.ds(2 * q, q)] if way == RIGHT else fr_ref.at[pl.ds(0, q)]
        else:
            part = 1 - way
            dst = last.at[way]
        return remote(ps_ref.at[s, pl.ds(part * q, q)], dst, rs_s.at[way, s], rs_r.at[way, s], to[way])

    def load_x(j, part):
        at = pl.ds(part * half, half)
        return pltpu.make_async_copy(g_ref.at[j - 1, at], xv.at[lax.rem(j, 2), at], lx.at[part])

    def load_own(i, part):
        src = xp_ref if part else x_ref
        return pltpu.make_async_copy(
            src.at[pl.ds(i * half, half)], xv.at[i, pl.ds(part * half, half)], lx.at[part]
        )

    def load_w(w_ref, part, n, sem):
        return pltpu.make_async_copy(
            w_ref.at[:, pl.ds(n * TN, TN)], wguv.at[n, :, pl.ds(part * TN, TN)], sem.at[n]
        )

    def load_wd(n):
        return pltpu.make_async_copy(wd_ref.at[:, pl.ds(n * TD, TD)], wdv.at[n], wd_sem.at[n])

    def load_gate_up(m):
        for i in range(UNROLL):
            load_w(wg_ref, 0, m * UNROLL + i, wg_sem).start()
            load_w(wu_ref, 1, m * UNROLL + i, wu_sem).start()

    def load_down(m):
        for i in range(UNROLL):
            load_wd(m * UNROLL + i).start()

    def keep_sum(s):
        return pltpu.make_async_copy(trecv.at[lax.rem(s + 1, 2)], ps_ref.at[s], ps_sem.at[0])

    def load_u(s):
        return pltpu.make_async_copy(u_ref.at[s], uv, u_sem.at[0])

    barrier = pltpu.get_barrier_semaphore()
    for other in (*to, partner):
        pl.semaphore_signal(barrier, inc=1, device_id={"tp": other}, device_id_type=MESH)
    load_own(0, 0).start()
    load_gate_up(0)
    pl.semaphore_wait(barrier, 3)
    for s in (0, 1):
        for way in (LEFT, RIGHT):
            ag(way, s).start()
        dx_own(s).start()
    dx_own(0).wait_recv()
    load_own(0, 1).start()
    load_gate_up(1)

    def columns(body):
        def step(c, _):
            body(pl.ds(pl.multiple_of(c * TD, TD), TD))
            return 0

        lax.fori_loop(0, d // TD, step, 0)

    def add_terms(j, upstream):
        def body(at):
            total = ownv[1, :, at] + trecv[lax.rem(j, 2), :, at].astype(F32)
            if upstream:
                total = total + uv[:, at].astype(F32)
            trecv[lax.rem(j, 2), :, at] = total.astype(BF16)

        columns(body)

    def add_own(i, part):
        def body(at):
            ownv[i, :, at] = ownv[i, :, at] + part(at).astype(F32)

        columns(body)

    def chunk(j, _):
        slot = lax.rem(j, 2)
        before = j - 1
        for part in range(2):
            at = pl.ds(part * half, half)
            pltpu.make_async_copy(g_ref.at[0, at], xv.at[slot, at], lx.at[part]).wait()

        def gate_up(m, _):
            @pl.when(j == 0)
            def _():
                for i in range(UNROLL):
                    load_w(wg_ref, 0, m * UNROLL + i, wg_sem).wait()
                    load_w(wu_ref, 1, m * UNROLL + i, wu_sem).wait()

                @pl.when(m + 2 < nt // UNROLL)
                def _():
                    load_gate_up(m + 2)

                @pl.when(m + 2 >= nt // UNROLL)
                def _():
                    load_down(m + 2 - nt // UNROLL)

            @pl.when(jnp.logical_and(m == 1, j >= 1))
            def _():
                dt(before).start()

            @pl.when(jnp.logical_and(m == 2, j >= 6))
            def _():
                for s in (2, 3):
                    @pl.when(j == s + 4)
                    def _():
                        for way in (LEFT, RIGHT):
                            rs(way, s).wait_recv()
                        load_u(s - 2).start()

            @pl.when(jnp.logical_and(m == 3, j >= 1))
            def _():
                dt(before).wait()

                @pl.when(j == 1)
                def _():
                    add_own(0, lambda at: trecv[0, :, at])

                @pl.when(jnp.logical_and(j > 1, j < 6))
                def _():
                    add_terms(before, False)

                @pl.when(j >= 6)
                def _():
                    load_u(0).wait()
                    add_terms(before, True)

            for i in range(UNROLL):
                n = m * UNROLL + i
                both = jnp.dot(xv[slot], wguv[n], preferred_element_type=F32)
                gate, up = both[:, :TN], both[:, TN:]
                h[:, pl.ds(pl.multiple_of(n * TN, TN), TN)] = (gate * jax.nn.sigmoid(gate) * up).astype(BF16)
            return 0

        lax.fori_loop(0, nt // UNROLL, gate_up, 0)

        def down(m, _):
            @pl.when(j == 0)
            def _():
                for i in range(UNROLL):
                    load_wd(m * UNROLL + i).wait()

                @pl.when(m + 2 < nd // UNROLL)
                def _():
                    load_down(m + 2)

            @pl.when(m == 0)
            def _():
                @pl.when(j < STAGES)
                def _():
                    for way in (LEFT, RIGHT):
                        ag_landed(way, j)
                    dx(j).start()
                    for s in (0, 1):
                        @pl.when(j == s)
                        def _():
                            for way in (LEFT, RIGHT):
                                ag(way, s + 2).start()

                    @pl.when(j == 1)
                    def _():
                        for s in (4, 5):
                            for way in (LEFT, RIGHT):
                                ag(way, s).start()

                    load_x(j + 1, 0).start()

                @pl.when(j == STAGES)
                def _():
                    load_own(1, 0).start()

                @pl.when(j >= 2)
                def _():
                    keep_sum(j - 2).start()

            @pl.when(jnp.logical_and(m == 1, j >= 2))
            def _():
                keep_sum(j - 2).wait()
                for at, stages in ((2, (0,)), (4, (2, 1)), (5, (3,)), (6, (4,)), (7, (5,))):
                    @pl.when(j == at)
                    def _():
                        for s in stages:
                            for way in (LEFT, RIGHT):
                                rs(way, s).start()

            @pl.when(m == 2)
            def _():
                @pl.when(j < STAGES)
                def _():
                    dx(j).wait_recv()
                    load_x(j + 1, 1).start()

                @pl.when(j == STAGES)
                def _():
                    dx_own(1).wait_recv()
                    load_own(1, 1).start()

            for i in range(UNROLL):
                n = m * UNROLL + i
                at = pl.ds(pl.multiple_of(n * TD, TD), TD)
                term = jnp.dot(h[...], wdv[n], preferred_element_type=F32)
                ownv[lax.min(j, 1), :, at] = term[:half]
                tsend[:, at] = term[half:].astype(BF16)
            return 0

        lax.fori_loop(0, nd // UNROLL, down, 0)
        return 0

    lax.fori_loop(0, CHUNKS, chunk, 0)

    def fetch(src, dst, i):
        return pltpu.make_async_copy(src, dst, lx.at[i])

    def finish(dst, acc, part, rows_at):
        def body(at):
            dst[:, at] = (ownv[acc, rows_at, at] + part(at).astype(F32)).astype(BF16)

        columns(body)

    top, bottom = pl.ds(0, q), pl.ds(q, q)
    first, second = pl.ds(0, half), pl.ds(half, half)

    for s in (0, 1):
        for way in (LEFT, RIGHT):
            rs(way, s).wait_recv()
    loads = fetch(fl_ref.at[first], xv.at[0, first], 0), fetch(fr_ref.at[second], xv.at[0, second], 1)
    for load in loads:
        load.start()
    for load in loads:
        load.wait()
    dt(CHUNKS - 1).start()
    add_own(0, lambda at: xv[0, first, at])
    add_own(1, lambda at: xv[0, second, at])
    dt(CHUNKS - 1).wait()
    add_own(1, lambda at: trecv[(CHUNKS - 1) % 2, :, at])

    for way in (LEFT, RIGHT):
        rs(way, 4).wait_recv()
    loads = fetch(fr_ref.at[top], xv.at[1, top], 0), fetch(fl_ref.at[pl.ds(half, q)], xv.at[1, bottom], 1)
    for load in loads:
        load.start()
    for load in loads:
        load.wait()
    finish(y_ref.at[0, top], 0, lambda at: xv[1, top, at], top)
    finish(y_ref.at[1, top], 1, lambda at: xv[1, bottom, at], top)

    for s in range(STAGES):
        for way in (LEFT, RIGHT):
            ag(way, s).wait_send()
        dx(s).wait_send()
    for i in range(2):
        dx_own(i).wait_send()
    for s in range(STAGES - 1):
        for way in (LEFT, RIGHT):
            rs(way, s).wait_send()
    for way in (LEFT, RIGHT):
        rs(way, 5).wait_recv()
        finish(y_ref.at[way, bottom], way, lambda at, way=way: last[way, :, at], bottom)
    for way in (LEFT, RIGHT):
        rs(way, 5).wait_send()


def solution(mesh):
    n_tp = mesh.shape["tp"]

    def step(x, w_gate, w_up, w_down):
        rows, d = x.shape
        f = w_gate.shape[1]
        half = rows // 2
        nt, nd = f // TN, d // TD
        shape = jax.ShapeDtypeStruct
        outs = [
            pltpu.VMEM((2, half, d), BF16),
            shape((rows, d), BF16),
            shape((rows, d), BF16),
            shape((STAGES, rows, d), BF16),
            shape((rows, d), BF16),
            shape((2, half, d), BF16),
            shape((STAGES, half, d), BF16),
        ]
        dma = pltpu.SemaphoreType.DMA
        y, *_ = pl.pallas_call(
            functools.partial(kernel, n_tp),
            out_shape=outs,
            in_specs=[pl.BlockSpec(memory_space=pl.ANY)] * 4,
            out_specs=[pl.BlockSpec(memory_space=pltpu.VMEM)] + [pl.BlockSpec(memory_space=pl.ANY)] * (len(outs) - 1),
            scratch_shapes=[
                pltpu.VMEM((2, rows, d), BF16),
                pltpu.VMEM((nt, d, 2 * TN), BF16),
                pltpu.VMEM((nd, f, TD), BF16),
                pltpu.VMEM((rows, f), BF16),
                pltpu.VMEM((2, half, d), F32),
                pltpu.VMEM((half, d), BF16),
                pltpu.VMEM((half, d), BF16),
                pltpu.VMEM((2, rows // 4, d), BF16),
                dma((2, STAGES)), dma((2, STAGES)),
                dma((CHUNKS,)), dma((CHUNKS,)),
                dma((CHUNKS,)), dma((CHUNKS,)),
                dma((2, STAGES)), dma((2, STAGES)),
                dma((2,)), dma((nt,)), dma((nt,)), dma((nd,)), dma((1,)), dma((1,)),
            ],
            compiler_params=pltpu.CompilerParams(
                collective_id=0, has_side_effects=True, vmem_limit_bytes=64900000
            ),
            name="mlp_block",
        )(x, w_gate, w_up, w_down)
        return y.reshape(rows, d)

    return jax.shard_map(
        step,
        mesh=mesh,
        in_specs=(P(("dp", "tp"), None), P(None, "tp"), P(None, "tp"), P("tp", None)),
        out_specs=P(("dp", "tp"), None),
        check_vma=False,
    )
```

```python
import functools

import jax
import jax.numpy as jnp
from jax import lax
from jax.experimental import pallas as pl
from jax.experimental.pallas import tpu as pltpu
from jax.sharding import PartitionSpec as P

MESH = pl.DeviceIdType.MESH
BF16, F32 = jnp.bfloat16, jnp.float32
LEFT, RIGHT = 0, 1
TN = 256
TD = 1024
UNROLL = 2

STAGES = 6
CHUNKS = STAGES + 2


def kernel(
    n_tp, x_ref, wg_ref, wu_ref, wd_ref,
    y_ref, fl_ref, fr_ref, g_ref, xp_ref, u_ref, ps_ref,
    xv, wguv, wdv, h, ownv, tsend, uv, last,
    ag_s, ag_r, dx_s, dx_r, dt_s, dt_r, rs_s, rs_r, lx, wg_sem, wu_sem, wd_sem, ps_sem, u_sem,
):
    me = lax.axis_index("tp")
    core = lax.rem(me, 2)
    partner = me + 1 - 2 * core
    to = (lax.rem(me + n_tp - 2, n_tp), lax.rem(me + 2, n_tp))
    rows, d = x_ref.shape
    half, q = rows // 2, rows // 4
    nt, nd = wguv.shape[0], wdv.shape[0]
    trecv = y_ref

    def remote(src, dst, send, recv, target):
        return pltpu.make_async_remote_copy(
            src_ref=src, dst_ref=dst, send_sem=send, recv_sem=recv, device_id={"tp": target}, device_id_type=MESH
        )

    def ag(way, s):
        if s in (0, 1):
            src = x_ref.at[pl.ds((s + 2 * way) * q, q)]
        elif s in (2, 3):
            src = g_ref.at[s - 2, pl.ds(way * q, q)]
        else:
            src = x_ref.at[pl.ds((s - 4 + 2 * (1 - way)) * q, q)]
        return remote(src, g_ref.at[s, pl.ds(way * q, q)], ag_s.at[way, s], ag_r.at[way, s], to[way])

    def ag_landed(way, s):
        at = g_ref.at[s, pl.ds(way * q, q)]
        remote(at, at, ag_s.at[way, s], ag_r.at[way, s], to[way]).wait_recv()

    def dx_own(i):
        at = pl.ds(i * half, half)
        return remote(x_ref.at[at], xp_ref.at[at], dx_s.at[STAGES + i], dx_r.at[STAGES + i], partner)

    def dx(s):
        return remote(
            g_ref.at[s, pl.ds(0, half)], g_ref.at[s, pl.ds(half, half)], dx_s.at[s], dx_r.at[s], partner
        )

    def dt(j):
        return remote(tsend, trecv.at[lax.rem(j, 2)], dt_s.at[j], dt_r.at[j], partner)

    def rs(way, s):
        if s in (0, 1):
            part = 1 - way
            dst = fl_ref.at[pl.ds(s * q, q)] if way == RIGHT else fr_ref.at[pl.ds((2 + s) * q, q)]
        elif s in (2, 3):
            part = way
            dst = u_ref.at[s - 2, pl.ds((1 - way) * q, q)]
        elif s == 4:
            part = 1 - way
            dst = fl_ref.at[pl.ds(2 * q, q)] if way == RIGHT else fr_ref.at[pl.ds(0, q)]
        else:
            part = 1 - way
            dst = last.at[way]
        return remote(ps_ref.at[s, pl.ds(part * q, q)], dst, rs_s.at[way, s], rs_r.at[way, s], to[way])

    def load_x(j, part):
        at = pl.ds(part * half, half)
        return pltpu.make_async_copy(g_ref.at[j - 1, at], xv.at[lax.rem(j, 2), at], lx.at[part])

    def load_own(i, part):
        src = xp_ref if part else x_ref
        return pltpu.make_async_copy(
            src.at[pl.ds(i * half, half)], xv.at[i, pl.ds(part * half, half)], lx.at[part]
        )

    def load_w(w_ref, part, n, sem):
        return pltpu.make_async_copy(
            w_ref.at[:, pl.ds(n * TN, TN)], wguv.at[n, :, pl.ds(part * TN, TN)], sem.at[n]
        )

    def load_wd(n):
        return pltpu.make_async_copy(wd_ref.at[:, pl.ds(n * TD, TD)], wdv.at[n], wd_sem.at[n])

    def load_gate_up(m):
        for i in range(UNROLL):
            load_w(wg_ref, 0, m * UNROLL + i, wg_sem).start()
            load_w(wu_ref, 1, m * UNROLL + i, wu_sem).start()

    def load_down(m):
        for i in range(UNROLL):
            load_wd(m * UNROLL + i).start()

    def keep_sum(s):
        return pltpu.make_async_copy(trecv.at[lax.rem(s + 1, 2)], ps_ref.at[s], ps_sem.at[0])

    def load_u(s):
        return pltpu.make_async_copy(u_ref.at[s], uv, u_sem.at[0])

    barrier = pltpu.get_barrier_semaphore()
    for other in (*to, partner):
        pl.semaphore_signal(barrier, inc=1, device_id={"tp": other}, device_id_type=MESH)
    load_own(0, 0).start()
    load_gate_up(0)
    pl.semaphore_wait(barrier, 3)
    for s in (0, 1):
        for way in (LEFT, RIGHT):
            ag(way, s).start()
        dx_own(s).start()
    dx_own(0).wait_recv()
    load_own(0, 1).start()
    load_gate_up(1)

    def columns(body):
        def step(c, _):
            body(pl.ds(pl.multiple_of(c * TD, TD), TD))
            return 0

        lax.fori_loop(0, d // TD, step, 0)

    def add_terms(j, upstream):
        def body(at):
            total = ownv[1, :, at] + trecv[lax.rem(j, 2), :, at].astype(F32)
            if upstream:
                total = total + uv[:, at].astype(F32)
            trecv[lax.rem(j, 2), :, at] = total.astype(BF16)

        columns(body)

    def add_own(i, part):
        def body(at):
            ownv[i, :, at] = ownv[i, :, at] + part(at).astype(F32)

        columns(body)

    def pass_on(j):
        for way in (LEFT, RIGHT):
            ag_landed(way, j)
        dx(j).start()
        for s in (0, 1):
            @pl.when(j == s)
            def _():
                for way in (LEFT, RIGHT):
                    ag(way, s + 2).start()

        @pl.when(j == 1)
        def _():
            for s in (4, 5):
                for way in (LEFT, RIGHT):
                    ag(way, s).start()

        load_x(j + 1, 0).start()

    def chunk(j, _):
        slot = lax.rem(j, 2)
        before = j - 1
        for part in range(2):
            at = pl.ds(part * half, half)
            pltpu.make_async_copy(g_ref.at[0, at], xv.at[slot, at], lx.at[part]).wait()

        def gate_up(m, _):
            @pl.when(j == 0)
            def _():
                for i in range(UNROLL):
                    load_w(wg_ref, 0, m * UNROLL + i, wg_sem).wait()
                    load_w(wu_ref, 1, m * UNROLL + i, wu_sem).wait()

                @pl.when(m + 2 < nt // UNROLL)
                def _():
                    load_gate_up(m + 2)

                @pl.when(m + 2 >= nt // UNROLL)
                def _():
                    load_down(m + 2 - nt // UNROLL)

            @pl.when(jnp.logical_and(m == 1, j >= 1))
            def _():
                dt(before).start()

            @pl.when(jnp.logical_and(m == 2, j >= 6))
            def _():
                for s in (2, 3):
                    @pl.when(j == s + 4)
                    def _():
                        for way in (LEFT, RIGHT):
                            rs(way, s).wait_recv()
                        load_u(s - 2).start()

            @pl.when(jnp.logical_and(m == 3, j >= 1))
            def _():
                dt(before).wait()

                @pl.when(j == 1)
                def _():
                    add_own(0, lambda at: trecv[0, :, at])

                @pl.when(jnp.logical_and(j > 1, j < 6))
                def _():
                    add_terms(before, False)

                @pl.when(j >= 6)
                def _():
                    load_u(0).wait()
                    add_terms(before, True)

            @pl.when(jnp.logical_and(m == 3, jnp.logical_and(j >= 1, j < STAGES)))
            def _():
                pass_on(j)

            for i in range(UNROLL):
                n = m * UNROLL + i
                both = jnp.dot(xv[slot], wguv[n], preferred_element_type=F32)
                gate, up = both[:, :TN], both[:, TN:]
                h[:, pl.ds(pl.multiple_of(n * TN, TN), TN)] = (gate * jax.nn.sigmoid(gate) * up).astype(BF16)
            return 0

        lax.fori_loop(0, nt // UNROLL, gate_up, 0)

        def down(m, _):
            @pl.when(j == 0)
            def _():
                for i in range(UNROLL):
                    load_wd(m * UNROLL + i).wait()

                @pl.when(m + 2 < nd // UNROLL)
                def _():
                    load_down(m + 2)

            @pl.when(m == 0)
            def _():
                @pl.when(j == 0)
                def _():
                    pass_on(jnp.int32(0))

                @pl.when(j == STAGES)
                def _():
                    load_own(1, 0).start()

                @pl.when(j >= 2)
                def _():
                    keep_sum(j - 2).start()

            @pl.when(jnp.logical_and(m == 1, j >= 2))
            def _():
                keep_sum(j - 2).wait()
                for at, stages in ((2, (0,)), (4, (2, 1)), (5, (3,)), (6, (4,)), (7, (5,))):
                    @pl.when(j == at)
                    def _():
                        for s in stages:
                            for way in (LEFT, RIGHT):
                                rs(way, s).start()

            @pl.when(m == 1)
            def _():
                @pl.when(j < STAGES)
                def _():
                    dx(j).wait_recv()
                    load_x(j + 1, 1).start()

                @pl.when(j == STAGES)
                def _():
                    dx_own(1).wait_recv()
                    load_own(1, 1).start()

            for i in range(UNROLL):
                n = m * UNROLL + i
                at = pl.ds(pl.multiple_of(n * TD, TD), TD)
                term = jnp.dot(h[...], wdv[n], preferred_element_type=F32)
                ownv[lax.min(j, 1), :, at] = term[:half]
                tsend[:, at] = term[half:].astype(BF16)
            return 0

        lax.fori_loop(0, nd // UNROLL, down, 0)
        return 0

    lax.fori_loop(0, CHUNKS, chunk, 0)

    def fetch(src, dst, i):
        return pltpu.make_async_copy(src, dst, lx.at[i])

    def finish(dst, acc, part, rows_at):
        def body(at):
            dst[:, at] = (ownv[acc, rows_at, at] + part(at).astype(F32)).astype(BF16)

        columns(body)

    top, bottom = pl.ds(0, q), pl.ds(q, q)
    first, second = pl.ds(0, half), pl.ds(half, half)

    for s in (0, 1):
        for way in (LEFT, RIGHT):
            rs(way, s).wait_recv()
    loads = fetch(fl_ref.at[first], xv.at[0, first], 0), fetch(fr_ref.at[second], xv.at[0, second], 1)
    for load in loads:
        load.start()
    for load in loads:
        load.wait()
    dt(CHUNKS - 1).start()
    add_own(0, lambda at: xv[0, first, at])
    add_own(1, lambda at: xv[0, second, at])
    dt(CHUNKS - 1).wait()
    add_own(1, lambda at: trecv[(CHUNKS - 1) % 2, :, at])

    for way in (LEFT, RIGHT):
        rs(way, 4).wait_recv()
    loads = fetch(fr_ref.at[top], xv.at[1, top], 0), fetch(fl_ref.at[pl.ds(half, q)], xv.at[1, bottom], 1)
    for load in loads:
        load.start()
    for load in loads:
        load.wait()
    finish(y_ref.at[0, top], 0, lambda at: xv[1, top, at], top)
    finish(y_ref.at[1, top], 1, lambda at: xv[1, bottom, at], top)

    for s in range(STAGES):
        for way in (LEFT, RIGHT):
            ag(way, s).wait_send()
        dx(s).wait_send()
    for i in range(2):
        dx_own(i).wait_send()
    for s in range(STAGES - 1):
        for way in (LEFT, RIGHT):
            rs(way, s).wait_send()
    for way in (LEFT, RIGHT):
        rs(way, 5).wait_recv()
        finish(y_ref.at[way, bottom], way, lambda at, way=way: last[way, :, at], bottom)
    for way in (LEFT, RIGHT):
        rs(way, 5).wait_send()


def solution(mesh):
    n_tp = mesh.shape["tp"]

    def step(x, w_gate, w_up, w_down):
        rows, d = x.shape
        f = w_gate.shape[1]
        half = rows // 2
        nt, nd = f // TN, d // TD
        shape = jax.ShapeDtypeStruct
        outs = [
            pltpu.VMEM((2, half, d), BF16),
            shape((rows, d), BF16),
            shape((rows, d), BF16),
            shape((STAGES, rows, d), BF16),
            shape((rows, d), BF16),
            shape((2, half, d), BF16),
            shape((STAGES, half, d), BF16),
        ]
        dma = pltpu.SemaphoreType.DMA
        y, *_ = pl.pallas_call(
            functools.partial(kernel, n_tp),
            out_shape=outs,
            in_specs=[pl.BlockSpec(memory_space=pl.ANY)] * 4,
            out_specs=[pl.BlockSpec(memory_space=pltpu.VMEM)] + [pl.BlockSpec(memory_space=pl.ANY)] * (len(outs) - 1),
            scratch_shapes=[
                pltpu.VMEM((2, rows, d), BF16),
                pltpu.VMEM((nt, d, 2 * TN), BF16),
                pltpu.VMEM((nd, f, TD), BF16),
                pltpu.VMEM((rows, f), BF16),
                pltpu.VMEM((2, half, d), F32),
                pltpu.VMEM((half, d), BF16),
                pltpu.VMEM((half, d), BF16),
                pltpu.VMEM((2, rows // 4, d), BF16),
                dma((2, STAGES)), dma((2, STAGES)),
                dma((CHUNKS,)), dma((CHUNKS,)),
                dma((CHUNKS,)), dma((CHUNKS,)),
                dma((2, STAGES)), dma((2, STAGES)),
                dma((2,)), dma((nt,)), dma((nt,)), dma((nd,)), dma((1,)), dma((1,)),
            ],
            compiler_params=pltpu.CompilerParams(
                collective_id=0, has_side_effects=True, vmem_limit_bytes=64900000
            ),
            name="mlp_block",
        )(x, w_gate, w_up, w_down)
        return y.reshape(rows, d)

    return jax.shard_map(
        step,
        mesh=mesh,
        in_specs=(P(("dp", "tp"), None), P(None, "tp"), P(None, "tp"), P("tp", None)),
        out_specs=P(("dp", "tp"), None),
        check_vma=False,
    )
```
